32 devices in a mesh: gx: 8 (over y, x, core), gy: 4 (over z).
Axes of the slice: x: 2, y: 2, z: 4, core: 2. Of those that a mesh axis runs over, the one named last changes fastest.
Arguments:
- adjoint: float32 [9, 32, 128, 512], P(None, 'gx', 'gy'), may hold values from -6 to 6
- buoyancy: float32 [32, 128, 512], P('gx', 'gy'), may hold values from 0.5 to 2
- lame_lambda: float32 [32, 128, 512], P('gx', 'gy'), may hold values from 0.5 to 2
- shear_mu: float32 [32, 128, 512], P('gx', 'gy'), may hold values from 0.3 to 1.2
- packed: int32 [8, 8, 4, 12, 2048], P('gx', None, 'gy'), may hold values from -2147483648 to 2147483646
- scales: float32 [8, 8, 4, 12], P('gx', None, 'gy'), may hold values from 0.005 to 0.05
- perm: int32 [8, 8], P('gx'), may hold values from 0 to 7, each once within a row
Outputs:
- adjoint_out: float32 [9, 32, 128, 512], P(None, 'gx', 'gy')
- gradients: float32 [2, 32, 128, 512], P(None, 'gx', 'gy')
The draws below stay inside these ranges and needn't reach their ends.
Inputs may be any that keep to these rules, and one draw needn't show every extreme that they name: Each row of perm names every number 0 to 7 once. The words of packed are stored inputs and may cross devices as they are, four signed bytes to a word; only values that a program computes travel in float32.
All inputs are finite; a program needn't handle non-finite values.
Results may differ from the reference program's by a relative error of at most 0.0003.
Values sent between devices are 32-bit elements; how exact they have to be, the bound alone decides.
A program may use at most 128 MiB of HBM per device.

```python
import math
import jax
import jax.numpy as jnp
from jax import lax

CX = 4
CY = 32
CZ = 512
STEPS = 2
COMP = 12
OWNERS = 8
SEGW = 2048
NX = 32
NY = 128
NZ = 512
N_GY = 4


def place_ends(values, key, low, top_value):
    longest = values.shape.index(max(values.shape))
    spots = []
    for shift in (0, 1):
        where = [jax.random.randint(jax.random.fold_in(key, axis), (), 0, length) for axis, length in enumerate(values.shape)]
        where[longest] = (where[longest] + shift) % values.shape[longest]
        spots.append(tuple(where))
    return values.at[spots[0]].set(low).at[spots[1]].set(top_value)


def steps_of(stream_key, extent, cuts, low, top_value):
    loudness = 1.0
    for position, parts in cuts:
        draws = jax.random.uniform(jax.random.fold_in(jax.random.fold_in(stream_key, 6), position), (parts,), jnp.float32, low / len(cuts), top_value / len(cuts))
        loudness = loudness * jnp.repeat(jnp.exp(draws), extent[position] // parts).reshape((-1,) + (1,) * (len(extent) - 1 - position))
    return loudness


def normal_values(own_key, shape, spread, bound, cuts=(), kind=jnp.bfloat16):
    values = jax.random.normal(own_key, shape, jnp.float32) * spread
    if len(cuts) > 0:
        values = steps_of(own_key, shape, cuts, -0.22, 0.18) * values
    return jnp.clip(values, min=-bound, max=bound).astype(kind)


def setup_inputs(seed: int = 0) -> dict:
    keys = jax.random.split(jax.random.key(seed), 8)
    adjoint = normal_values(keys[0], (9, NX, NY, NZ), 1.0, 6.0, ((1, 8), (2, 4)), jnp.float32)
    buoyancy = jnp.clip(jnp.exp(math.log(2.0) - 1.3862944 * jax.random.uniform(keys[1], (NX, NY, NZ), jnp.float32) ** steps_of(keys[1], (NX, NY, NZ), ((0, 8), (1, 4)), -0.2, 0.2)), 0.5, 2.0)
    lame_lambda = jnp.clip(jnp.exp(math.log(2.0) - 1.3862944 * jax.random.uniform(keys[2], (NX, NY, NZ), jnp.float32) ** steps_of(keys[2], (NX, NY, NZ), ((0, 8), (1, 4)), -0.2, 0.2)), 0.5, 2.0)
    shear_mu = jnp.clip(jnp.exp(math.log(1.2) - 1.3862944 * jax.random.uniform(keys[3], (NX, NY, NZ), jnp.float32) ** steps_of(keys[3], (NX, NY, NZ), ((0, 8), (1, 4)), -0.2, 0.2)), 0.3, 1.2)
    packed = place_ends(jax.random.randint(keys[4], (OWNERS, OWNERS, N_GY, COMP, SEGW), -2147483648, 2147483647), jax.random.fold_in(keys[4], 1), -2147483648, 2147483646).astype(jnp.int32)
    scales = jnp.clip(jnp.exp(math.log(0.05) - 2.3025851 * jax.random.uniform(keys[5], (OWNERS, OWNERS, N_GY, COMP), jnp.float32) ** steps_of(keys[5], (OWNERS, OWNERS, N_GY, COMP), ((0, 8), (2, 4)), -0.2, 0.2)), 0.005, 0.05)
    perm = jax.vmap(lambda own: jax.random.permutation(own, OWNERS))(jax.random.split(keys[6], OWNERS)).reshape((OWNERS, OWNERS)).astype(jnp.int32)
    return dict(adjoint=adjoint, buoyancy=buoyancy, lame_lambda=lame_lambda, shear_mu=shear_mu, packed=packed, scales=scales, perm=perm)


courant = 0.15


def unpack(words):
    low = (words & 255) - 128
    middle = (jnp.right_shift(words, 8) & 255) - 128
    high = (jnp.right_shift(words, 16) & 255) - 128
    topmost = jnp.right_shift(words, 24)
    return jnp.concatenate([low, middle, high, topmost], axis=-1).astype(jnp.float32)


def inverse_order(row):
    count = row.shape[0]
    slots = jnp.arange(count, dtype=jnp.int32)
    hits = (row[None, :] == slots[:, None]).astype(jnp.int32)
    return jnp.sum(hits * slots[None, :], axis=1).astype(jnp.int32)


def forward_field(packed, scales, perm):
    comp = packed.shape[3]
    by_owner = jnp.swapaxes(packed, 0, 1)
    factors = jnp.swapaxes(scales, 0, 1)

    def one_owner(items):
        words, factor, row = items
        blocks = unpack(words) * factor[..., None]
        ordered = jnp.take(blocks, inverse_order(row), axis=0)
        return jnp.transpose(ordered, (2, 1, 0, 3)).reshape(comp, N_GY, CX, CY, CZ)

    whole_field = lax.map(one_owner, (by_owner, factors, perm))
    whole_field = jnp.transpose(whole_field, (1, 0, 3, 2, 4, 5))
    return whole_field.reshape(comp, NX, NY, NZ)


def step_ahead(field, axis):
    count = field.shape[axis]
    widths = [(0, 0)] * field.ndim
    widths[axis] = (0, 1)
    return jnp.pad(lax.slice_in_dim(field, 1, count, axis=axis), widths)


def step_behind(field, axis):
    count = field.shape[axis]
    widths = [(0, 0)] * field.ndim
    widths[axis] = (1, 0)
    return jnp.pad(lax.slice_in_dim(field, 0, count - 1, axis=axis), widths)


def diff_ahead(field, axis):
    return step_ahead(field, axis) - field


def diff_behind(field, axis):
    return field - step_behind(field, axis)


def move_velocity(velocity, stress, buoyancy):
    scaled = courant * buoyancy
    return [
        velocity[0] - scaled * (diff_ahead(stress[0], 0) + diff_behind(stress[3], 1) + diff_behind(stress[4], 2)),
        velocity[1] - scaled * (diff_behind(stress[3], 0) + diff_ahead(stress[1], 1) + diff_behind(stress[5], 2)),
        velocity[2] - scaled * (diff_behind(stress[4], 0) + diff_behind(stress[5], 1) + diff_ahead(stress[2], 2)),
    ]


def strains(velocity):
    return [
        diff_behind(velocity[0], 0),
        diff_behind(velocity[1], 1),
        diff_behind(velocity[2], 2),
        diff_ahead(velocity[0], 1) + diff_ahead(velocity[1], 0),
        diff_ahead(velocity[0], 2) + diff_ahead(velocity[2], 0),
        diff_ahead(velocity[1], 2) + diff_ahead(velocity[2], 1),
    ]


def move_stress(stress, strain, lame_lambda, shear_mu):
    trace = strain[0] + strain[1] + strain[2]
    result = []
    for index in range(3):
        result.append(stress[index] - courant * (lame_lambda * trace + 2.0 * shear_mu * strain[index]))
    for index in range(3, 6):
        result.append(stress[index] - courant * shear_mu * strain[index])
    return result


def reference(adjoint, buoyancy, lame_lambda, shear_mu, packed, scales, perm):
    forward = forward_field(packed, scales, perm)
    velocity = [adjoint[index] for index in range(3)]
    stress = [adjoint[index] for index in range(3, 9)]
    grad_lambda = jnp.zeros(buoyancy.shape, jnp.float32)
    grad_mu = jnp.zeros(buoyancy.shape, jnp.float32)
    for step in range(STEPS):
        velocity = move_velocity(velocity, stress, buoyancy)
        strain = strains(velocity)
        stress = move_stress(stress, strain, lame_lambda, shear_mu)
        stored = [forward[6 * step + index] for index in range(6)]
        trace = strain[0] + strain[1] + strain[2]
        grad_lambda = grad_lambda + trace * (stored[0] + stored[1] + stored[2])
        grad_mu = grad_mu + 2.0 * (strain[0] * stored[0] + strain[1] * stored[1] + strain[2] * stored[2])
        grad_mu = grad_mu + strain[3] * stored[3] + strain[4] * stored[4] + strain[5] * stored[5]
    return jnp.stack(velocity + stress), jnp.stack([grad_lambda, grad_mu])
```

```python
import functools

import jax
import jax.numpy as jnp
from jax import lax
from jax.experimental import pallas as pl
from jax.experimental.pallas import tpu as pltpu
from jax.sharding import PartitionSpec as P

MESH = pl.DeviceIdType.MESH
STEPS = 2
COURANT = 0.15
ROWS = 8

VX, VY, VZ, SXX, SYY, SZZ, SXY, SXZ, SYZ = range(9)

STRESS_X = ((SXX, -1), (SXY, 1), (SXZ, 1))
STRESS_Y = ((SYY, -1), (SXY, 1), (SYZ, 1))
SPEED_X = ((VY, -1), (VZ, -1), (VX, 1))
SPEED_Y = ((VX, -1), (VZ, -1), (VY, 1))


def partner(me, distance, count):
    if count & (count - 1):
        return lax.rem(me + distance, count)
    result, bit = me, 1
    while bit < count:
        if distance & bit:
            result = result + bit - 2 * bit * ((me // bit) % 2)
        bit *= 2
    return result


def kernel(n_x, n_y, adj, buoy, lam, shear, packed, scales, perm, out, grads,
           cur, coef, strain, gsum, halo_x, halo_y, send_y, words, factors, factor_s, inv,
           in_sem, out_sem, xs_sem, xr_sem, ys_sem, yr_sem, ws_sem, wr_sem, fs_sem, fr_sem, loc_sem):
    cx, cy, cz = buoy.shape
    comp = packed.shape[1]
    lanes = packed.shape[3]
    segw = packed.shape[2] * lanes
    tiles = cy // ROWS
    me_x, me_y = lax.axis_index("gx"), lax.axis_index("gy")

    loads = []
    for index in (SXX, SXY, SXZ, SYY, SYZ, SZZ, VX, VY, VZ):
        loads.append(pltpu.make_async_copy(adj.at[index], cur.at[index, pl.ds(1, cx)], in_sem.at[index]))
    for index, ref in enumerate((buoy, lam, shear)):
        loads.append(pltpu.make_async_copy(ref, coef.at[index], in_sem.at[9 + index]))
    own_words = pltpu.make_async_copy(packed.at[me_x], words.at[me_x], loc_sem.at[0])
    own_factor = pltpu.make_async_copy(scales.at[0, me_x], factors.at[me_x], loc_sem.at[1])
    for copy in loads:
        copy.start()
    own_words.start()
    own_factor.start()

    barrier = pltpu.get_barrier_semaphore()
    for distance in range(1, n_x):
        pl.semaphore_signal(barrier, inc=1, device_id={"gx": partner(me_x, distance, n_x)}, device_id_type=MESH)

    def edge(way, axis):
        me, count = (me_x, n_x) if axis == "gx" else (me_y, n_y)
        return (me > 0) if way < 0 else (me < count - 1)

    for way in (-1, 1):
        @pl.when(edge(way, "gy"))
        def _():
            pl.semaphore_signal(barrier, inc=1, device_id={"gy": me_y + way}, device_id_type=MESH)

    pl.semaphore_wait(barrier, n_x - 1 + jnp.minimum(me_y, 1) + jnp.minimum(n_y - 1 - me_y, 1))

    def copy_x(step, kind, field, way, source):
        slot = 6 * step + kind
        return pltpu.make_async_remote_copy(
            src_ref=source, dst_ref=halo_x.at[slot], send_sem=xs_sem.at[slot], recv_sem=xr_sem.at[slot],
            device_id={"gx": me_x + way}, device_id_type=MESH)

    def copy_y(step, kind, way):
        slot = 6 * step + kind
        return pltpu.make_async_remote_copy(
            src_ref=send_y.at[slot], dst_ref=halo_y.at[slot], send_sem=ys_sem.at[slot], recv_sem=yr_sem.at[slot],
            device_id={"gy": me_y + way}, device_id_type=MESH)

    def layer(field, way):
        return cur.at[field, 1 if way < 0 else cx]

    def word_copy(distance):
        to = partner(me_x, distance, n_x)
        return pltpu.make_async_remote_copy(
            src_ref=packed.at[to], dst_ref=words.at[me_x], send_sem=ws_sem.at[distance],
            recv_sem=wr_sem.at[distance], device_id={"gx": to}, device_id_type=MESH)

    def factor_copy(distance):
        to = partner(me_x, distance, n_x)
        return pltpu.make_async_remote_copy(
            src_ref=scales.at[0, to], dst_ref=factors.at[me_x], send_sem=fs_sem.at[distance],
            recv_sem=fr_sem.at[distance], device_id={"gx": to}, device_id_type=MESH)

    def send_x(step, base, kinds, source, ways):
        for offset, (field, way) in enumerate(kinds):
            if way in ways:
                @pl.when(edge(way, "gx"))
                def _():
                    copy_x(step, base + offset, field, way, source(field, way)).start()

    def pack_rows(step, base, kinds):
        for offset, (field, way) in enumerate(kinds):
            row = 0 if way < 0 else cy - 1
            for x in range(cx):
                send_y[6 * step + base + offset, pl.ds(x, 1), :] = cur[field, 1 + x, pl.ds(row, 1), :]

    def send_rows(step, base, kinds):
        pack_rows(step, base, kinds)
        for offset, (field, way) in enumerate(kinds):
            @pl.when(edge(way, "gy"))
            def _():
                copy_y(step, base + offset, way).start()

    def finish_sends(step, base, kinds_x, kinds_y):
        for offset, (field, way) in enumerate(kinds_x):
            @pl.when(edge(way, "gx"))
            def _():
                copy_x(step, base + offset, field, way, layer(field, way)).wait_send()
        for offset, (field, way) in enumerate(kinds_y):
            @pl.when(edge(way, "gy"))
            def _():
                copy_y(step, base + offset, way).wait_send()

    def receive(step, base, kinds_x, kinds_y):
        for offset, (field, way) in enumerate(kinds_y):
            slot = 6 * step + base + offset

            @pl.when(edge(-way, "gy"))
            def _():
                copy_y(step, base + offset, way).wait_recv()

            @pl.when(jnp.logical_not(edge(-way, "gy")))
            def _():
                halo_y[slot] = jnp.zeros((cx, cz), jnp.float32)
        for offset, (field, way) in enumerate(kinds_x):
            slot = 6 * step + base + offset
            place = cx + 1 if way < 0 else 0

            @pl.when(edge(-way, "gx"))
            def _():
                copy_x(step, base + offset, field, way, layer(field, way)).wait_recv()
                cur[field, place] = halo_x[slot]

            @pl.when(jnp.logical_not(edge(-way, "gx")))
            def _():
                cur[field, place] = jnp.zeros((cy, cz), jnp.float32)

    groups = [[], [], [], []]
    half = max(n_x // 2, 1)
    for distance in range(1, n_x):
        if distance >= half:
            where = 0 if n_x < 8 else (1 if distance == half else 2 + (distance % 2))
        else:
            where = distance % 2
        if n_x == 8:
            where = {1: 0, 2: 0, 4: 0, 3: 1, 5: 1, 6: 2, 7: 3}[distance]
        groups[where].append(distance)

    def send_group(which):
        for distance in groups[which]:
            factor_copy(distance).start()
            word_copy(distance).start()

    sub = lax.broadcasted_iota(jnp.int32, (ROWS, cz), 0)
    lane = lax.broadcasted_iota(jnp.int32, (ROWS, cz), 1)
    first_row, last_row = sub == 0, sub == ROWS - 1
    first_lane, last_lane = lane == 0, lane == cz - 1

    def tile(field, x, t):
        return cur[field, x + 1, pl.ds(t * ROWS, ROWS), :]

    def z_before(value):
        return jnp.where(first_lane, 0.0, pltpu.roll(value, 1, 1))

    def z_after(value):
        return jnp.where(last_lane, 0.0, pltpu.roll(value, cz - 1, 1))

    def y_before(value, field, x, t, slot):
        row = halo_y[slot, pl.ds(x, 1), :] if t == 0 else cur[field, x + 1, pl.ds(t * ROWS - 1, 1), :]
        return jnp.where(first_row, jnp.broadcast_to(row, value.shape), pltpu.roll(value, 1, 0))

    def y_after(value, field, x, t, slot):
        row = halo_y[slot, pl.ds(x, 1), :] if t == tiles - 1 else cur[field, x + 1, pl.ds(t * ROWS + ROWS, 1), :]
        return jnp.where(last_row, jnp.broadcast_to(row, value.shape), pltpu.roll(value, ROWS - 1, 0))

    def velocity(step, x):
        slot = 6 * step
        for t in range(tiles):
            rows = pl.ds(t * ROWS, ROWS)
            scaled = COURANT * coef[0, x, rows, :]
            sxy, sxz, syz = tile(SXY, x, t), tile(SXZ, x, t), tile(SYZ, x, t)
            sxx, syy, szz = tile(SXX, x, t), tile(SYY, x, t), tile(SZZ, x, t)
            cur[VX, x + 1, rows, :] = tile(VX, x, t) - scaled * (
                (tile(SXX, x + 1, t) - sxx) + (sxy - y_before(sxy, SXY, x, t, slot + 1)) + (sxz - z_before(sxz)))
            cur[VY, x + 1, rows, :] = tile(VY, x, t) - scaled * (
                (sxy - tile(SXY, x - 1, t)) + (y_after(syy, SYY, x, t, slot) - syy) + (syz - z_before(syz)))
            cur[VZ, x + 1, rows, :] = tile(VZ, x, t) - scaled * (
                (sxz - tile(SXZ, x - 1, t)) + (syz - y_before(syz, SYZ, x, t, slot + 2)) + (z_after(szz) - szz))

    def stress(step, x):
        slot = 6 * step + 3
        for t in range(tiles):
            rows = pl.ds(t * ROWS, ROWS)
            vx, vy, vz = tile(VX, x, t), tile(VY, x, t), tile(VZ, x, t)
            exx = vx - tile(VX, x - 1, t)
            eyy = vy - y_before(vy, VY, x, t, slot + 2)
            ezz = vz - z_before(vz)
            exy = (y_after(vx, VX, x, t, slot) - vx) + (tile(VY, x + 1, t) - vy)
            exz = (z_after(vx) - vx) + (tile(VZ, x + 1, t) - vz)
            eyz = (z_after(vy) - vy) + (y_after(vz, VZ, x, t, slot + 1) - vz)
            both = (exx, eyy, ezz, exy, exz, eyz)
            for index, value in enumerate(both):
                strain[6 * step + index, x, rows, :] = value
            pull = (COURANT * coef[1, x, rows, :]) * (exx + eyy + ezz)
            mu = COURANT * coef[2, x, rows, :]
            for index in range(3):
                cur[SXX + index, x + 1, rows, :] = tile(SXX + index, x, t) - (pull + (2.0 * mu) * both[index])
            for index in range(3, 6):
                cur[SXX + index, x + 1, rows, :] = tile(SXX + index, x, t) - mu * both[index]

    def over(first, last, body):
        def run(x, carry):
            body(x)
            return carry
        lax.fori_loop(first, last, run, 0)

    def ends(body):
        def run(index, carry):
            body(index * (cx - 1))
            return carry
        lax.fori_loop(0, 2, run, 0)

    for step in range(STEPS):
        if step == 0:
            send_x(0, 0, STRESS_X, lambda field, way: adj.at[field, 0 if way < 0 else cx - 1], (-1, 1))
            for copy in loads:
                copy.wait()
            send_rows(0, 0, STRESS_Y)
            send_group(0)
            def invert(block, carry):
                total = jnp.int32(0)
                for holder in range(n_x):
                    total = jnp.where(perm[0, holder] == block, holder, total)
                inv[block] = total
                return carry
            lax.fori_loop(0, n_x, invert, 0)
        receive(step, 0, STRESS_X, STRESS_Y)
        if step > 0:
            finish_sends(step - 1, 3, SPEED_X, SPEED_Y)
        ends(functools.partial(velocity, step))
        send_x(step, 3, SPEED_X, layer, (-1, 1))
        over(1, cx - 1, functools.partial(velocity, step))
        send_rows(step, 3, SPEED_Y)
        send_group(1 + 2 * step)
        if step == STEPS - 1:
            speed_out = [pltpu.make_async_copy(cur.at[f, pl.ds(1, cx)], out.at[f], out_sem.at[f]) for f in range(3)]
            for copy in speed_out:
                copy.start()
        receive(step, 3, SPEED_X, SPEED_Y)
        finish_sends(step, 0, STRESS_X, STRESS_Y)
        ends(functools.partial(stress, step))
        if step < STEPS - 1:
            send_x(step + 1, 0, STRESS_X, layer, (-1, 1))
        over(1, cx - 1, functools.partial(stress, step))
        if step < STEPS - 1:
            send_rows(step + 1, 0, STRESS_Y)
            send_group(2 + 2 * step)
    finish_sends(STEPS - 1, 3, SPEED_X, SPEED_Y)
    stress_out = [pltpu.make_async_copy(cur.at[f, pl.ds(1, cx)], out.at[f], out_sem.at[f]) for f in range(3, 9)]
    for copy in stress_out:
        copy.start()

    own_words.wait()
    own_factor.wait()
    for distance in range(1, n_x):
        factor_copy(distance).wait()
    to_scalar = pltpu.make_async_copy(factors, factor_s, loc_sem.at[2])
    to_scalar.start()
    for distance in range(1, n_x):
        word_copy(distance).wait()
    to_scalar.wait()

    width = lanes
    per_x = cy * cz // (4 * segw)

    def source(row, chunk):
        offset = row * cz + chunk * width
        within = offset % (4 * segw)
        return offset // (4 * segw), within % segw, within // segw

    sub_w = lax.broadcasted_iota(jnp.int32, (ROWS, width), 0)

    def gradient(x):
        made = {}
        for t in range(tiles):
            for chunk in range(cz // width):
                rows = pl.ds(t * ROWS, ROWS)
                columns = pl.ds(chunk * width, width)
                plan = [source(t * ROWS + r, chunk) for r in range(ROWS)]
                shift = jnp.full((ROWS, width), 8 * plan[0][2], jnp.int32)
                for r in range(1, ROWS):
                    if plan[r][2] != plan[r - 1][2]:
                        shift = jnp.where(sub_w >= r, 8 * plan[r][2], shift)
                key = tuple(p[:2] for p in plan)
                distinct = list(dict.fromkeys(key))
                masks = []
                for item in distinct[1:]:
                    mask = None
                    for r in range(ROWS):
                        if key[r] == item:
                            mask = (sub_w == r) if mask is None else mask | (sub_w == r)
                    masks.append(mask)
                holders = {b: inv[x * per_x + b] for b in dict.fromkeys(k[0] for k in key)}
                blocks = [k[0] for k in key]

                def stored(c):
                    if (key, c) not in made:
                        word = None
                        for position, (block, start) in enumerate(distinct):
                            piece = jnp.broadcast_to(
                                words[holders[block], c, pl.ds(start // lanes, 1), :], (ROWS, width))
                            word = piece if word is None else jnp.where(masks[position - 1], piece, word)
                        made[key, c] = word ^ jnp.int32(-2147483648)
                    byte = (lax.shift_right_logical(made[key, c], shift) & 255) - 128
                    factor = None
                    for r in range(ROWS):
                        if r == 0:
                            factor = factor_s[holders[blocks[0]], 0, c]
                        elif blocks[r] != blocks[r - 1]:
                            factor = jnp.where(sub_w >= r, factor_s[holders[blocks[r]], 0, c], factor)
                    return byte.astype(jnp.float32) * factor

                grad_lambda = jnp.zeros((ROWS, width), jnp.float32)
                grad_mu = jnp.zeros((ROWS, width), jnp.float32)
                for step in range(comp // 6):
                    e = [strain[6 * step + index, x, rows, columns] for index in range(6)]
                    f = [stored(6 * step + index) for index in range(6)]
                    grad_lambda = grad_lambda + (e[0] + e[1] + e[2]) * (f[0] + f[1] + f[2])
                    grad_mu = grad_mu + 2.0 * (e[0] * f[0] + e[1] * f[1] + e[2] * f[2])
                    grad_mu = grad_mu + e[3] * f[3] + e[4] * f[4] + e[5] * f[5]
                gsum[0, x, rows, columns] = grad_lambda
                gsum[1, x, rows, columns] = grad_mu

    over(0, cx, gradient)
    grad_out = pltpu.make_async_copy(gsum, grads, loc_sem.at[3])
    grad_out.start()
    for copy in speed_out + stress_out:
        copy.wait()
    grad_out.wait()


def on_device(n_x, n_y, adjoint, buoyancy, lame_lambda, shear_mu, packed, scales, perm):
    fields, cx, cy, cz = adjoint.shape
    comp, segw = packed.shape[3:]
    lanes = min(128, segw)
    packed = packed.reshape(n_x, comp, segw // lanes, lanes)
    halos = 6 * STEPS
    dma = pltpu.SemaphoreType.DMA
    any_space = pl.BlockSpec(memory_space=pl.ANY)
    return pl.pallas_call(
        functools.partial(kernel, n_x, n_y),
        out_shape=(jax.ShapeDtypeStruct(adjoint.shape, jnp.float32),
                   jax.ShapeDtypeStruct((2, cx, cy, cz), jnp.float32)),
        in_specs=[pl.BlockSpec(memory_space=pltpu.HBM)] * 6 + [pl.BlockSpec(memory_space=pltpu.SMEM)],
        out_specs=(any_space, any_space),
        scratch_shapes=[
            pltpu.VMEM((fields, cx + 2, cy, cz), jnp.float32),
            pltpu.VMEM((3, cx, cy, cz), jnp.float32),
            pltpu.VMEM((comp, cx, cy, cz), jnp.float32),
            pltpu.VMEM((2, cx, cy, cz), jnp.float32),
            pltpu.VMEM((halos, cy, cz), jnp.float32),
            pltpu.VMEM((halos, cx, cz), jnp.float32),
            pltpu.VMEM((halos, cx, cz), jnp.float32),
            pltpu.VMEM((n_x, comp, segw // lanes, lanes), jnp.int32),
            pltpu.VMEM((n_x, 1, comp), jnp.float32),
            pltpu.SMEM((n_x, 1, comp), jnp.float32),
            pltpu.SMEM((n_x,), jnp.int32),
            dma((12,)), dma((9,)), dma((halos,)), dma((halos,)), dma((halos,)), dma((halos,)),
            dma((n_x,)), dma((n_x,)), dma((n_x,)), dma((n_x,)), dma((4,)),
        ],
        compiler_params=pltpu.CompilerParams(collective_id=0, has_side_effects=True,
                                             vmem_limit_bytes=40 * 1024 * 1024),
    )(adjoint, buoyancy, lame_lambda, shear_mu, packed, scales, perm)


def solution(mesh):
    return jax.shard_map(
        functools.partial(on_device, mesh.shape["gx"], mesh.shape["gy"]),
        mesh=mesh,
        in_specs=(
            P(None, "gx", "gy", None),
            P("gx", "gy", None),
            P("gx", "gy", None),
            P("gx", "gy", None),
            P("gx", None, "gy", None, None),
            P("gx", None, "gy", None),
            P("gx", None),
        ),
        out_specs=(P(None, "gx", "gy", None), P(None, "gx", "gy", None)),
        check_vma=False,
    )
```

```python
import functools

import jax
import jax.numpy as jnp
from jax import lax
from jax.experimental import pallas as pl
from jax.experimental.pallas import tpu as pltpu
from jax.sharding import PartitionSpec as P

MESH = pl.DeviceIdType.MESH
STEPS = 2
COURANT = 0.15
ROWS = 8

VX, VY, VZ, SXX, SYY, SZZ, SXY, SXZ, SYZ = range(9)

STRESS_X = ((0, (SXX,), -1), (1, (SXY, SXZ), 1))
STRESS_Y = ((0, (SYY,), -1), (1, (SXY, SYZ), 1))
SPEED_X = ((3, (VY, VZ), -1), (5, (VX,), 1))
SPEED_Y = ((3, (VX, VZ), -1), (5, (VY,), 1))


def partner(me, distance, count):
    if count & (count - 1):
        return lax.rem(me + distance, count)
    result, bit = me, 1
    while bit < count:
        if distance & bit:
            result = result + bit - 2 * bit * ((me // bit) % 2)
        bit *= 2
    return result


def kernel(n_x, n_y, adj, buoy, lam, shear, packed, scales, perm, out, grads,
           cur, coef, strain, halo_x, halo_y, send_y, words, factors, factor_s, inv,
           in_sem, xs_sem, xr_sem, ys_sem, yr_sem, ws_sem, wr_sem, fs_sem, fr_sem, loc_sem):
    cx, cy, cz = buoy.shape
    comp = packed.shape[1]
    lanes = packed.shape[3]
    segw = packed.shape[2] * lanes
    tiles = cy // ROWS
    me_x, me_y = lax.axis_index("gx"), lax.axis_index("gy")

    loads = []
    for index in (SXX, SXY, SXZ, SYY, SYZ, SZZ, VX, VY, VZ):
        loads.append(pltpu.make_async_copy(adj.at[index], cur.at[index, pl.ds(1, cx)], in_sem.at[index]))
    for index, ref in enumerate((buoy, lam, shear)):
        loads.append(pltpu.make_async_copy(ref, coef.at[index], in_sem.at[9 + index]))
    own_words = pltpu.make_async_copy(packed.at[me_x], words.at[me_x], loc_sem.at[0])
    own_factor = pltpu.make_async_copy(scales.at[0, me_x], factors.at[me_x], loc_sem.at[1])
    for copy in loads:
        copy.start()
    own_words.start()
    own_factor.start()

    barrier = pltpu.get_barrier_semaphore()
    for distance in range(1, n_x):
        pl.semaphore_signal(barrier, inc=1, device_id={"gx": partner(me_x, distance, n_x)}, device_id_type=MESH)

    def edge(way, axis):
        me, count = (me_x, n_x) if axis == "gx" else (me_y, n_y)
        return (me > 0) if way < 0 else (me < count - 1)

    for way in (-1, 1):
        @pl.when(edge(way, "gy"))
        def _():
            pl.semaphore_signal(barrier, inc=1, device_id={"gy": me_y + way}, device_id_type=MESH)

    pl.semaphore_wait(barrier, n_x - 1 + jnp.minimum(me_y, 1) + jnp.minimum(n_y - 1 - me_y, 1))

    def copy_x(step, message, source):
        start, fields, way = message
        slot = 6 * step + start
        return pltpu.make_async_remote_copy(
            src_ref=source(fields, way), dst_ref=halo_x.at[pl.ds(slot, len(fields))],
            send_sem=xs_sem.at[slot], recv_sem=xr_sem.at[slot],
            device_id={"gx": me_x + way}, device_id_type=MESH)

    def copy_y(step, message):
        start, fields, way = message
        slot = 6 * step + start
        return pltpu.make_async_remote_copy(
            src_ref=send_y.at[pl.ds(slot, len(fields))], dst_ref=halo_y.at[pl.ds(slot, len(fields))],
            send_sem=ys_sem.at[slot], recv_sem=yr_sem.at[slot],
            device_id={"gy": me_y + way}, device_id_type=MESH)

    def layer(fields, way):
        return cur.at[pl.ds(fields[0], len(fields)), 1 if way < 0 else cx]

    def first_layer(fields, way):
        return adj.at[pl.ds(fields[0], len(fields)), 0 if way < 0 else cx - 1]

    def word_copy(distance):
        to = partner(me_x, distance, n_x)
        return pltpu.make_async_remote_copy(
            src_ref=packed.at[to], dst_ref=words.at[me_x], send_sem=ws_sem.at[distance],
            recv_sem=wr_sem.at[distance], device_id={"gx": to}, device_id_type=MESH)

    def factor_copy(distance):
        to = partner(me_x, distance, n_x)
        return pltpu.make_async_remote_copy(
            src_ref=scales.at[0, to], dst_ref=factors.at[me_x], send_sem=fs_sem.at[distance],
            recv_sem=fr_sem.at[distance], device_id={"gx": to}, device_id_type=MESH)

    def send_x(step, messages, source):
        for message in messages:
            @pl.when(edge(message[2], "gx"))
            def _():
                copy_x(step, message, source).start()

    def send_rows(step, messages):
        for message in messages:
            start, fields, way = message

            @pl.when(edge(way, "gy"))
            def _():
                row = 0 if way < 0 else cy - 1
                for offset, field in enumerate(fields):
                    for x in range(cx):
                        send_y[6 * step + start + offset, pl.ds(x, 1), :] = cur[field, 1 + x, pl.ds(row, 1), :]
                copy_y(step, message).start()

    def finish_sends(step, messages_x, messages_y):
        for message in messages_x:
            @pl.when(edge(message[2], "gx"))
            def _():
                copy_x(step, message, layer).wait_send()
        for message in messages_y:
            @pl.when(edge(message[2], "gy"))
            def _():
                copy_y(step, message).wait_send()

    def receive(step, messages_x, messages_y):
        for message in messages_y:
            start, fields, way = message

            @pl.when(edge(-way, "gy"))
            def _():
                copy_y(step, message).wait_recv()

            @pl.when(jnp.logical_not(edge(-way, "gy")))
            def _():
                for offset in range(len(fields)):
                    halo_y[6 * step + start + offset] = jnp.zeros((cx, cz), jnp.float32)
        for message in messages_x:
            start, fields, way = message
            place = cx + 1 if way < 0 else 0

            @pl.when(edge(-way, "gx"))
            def _():
                copy_x(step, message, layer).wait_recv()
                for offset, field in enumerate(fields):
                    cur[field, place] = halo_x[6 * step + start + offset]

            @pl.when(jnp.logical_not(edge(-way, "gx")))
            def _():
                for field in fields:
                    cur[field, place] = jnp.zeros((cy, cz), jnp.float32)

    groups = [[], [], [], []]
    half = max(n_x // 2, 1)
    for distance in range(1, n_x):
        if distance >= half:
            where = 0 if n_x < 8 else (1 if distance == half else 2 + (distance % 2))
        else:
            where = distance % 2
        if n_x == 8:
            where = {1: 0, 2: 0, 4: 0, 3: 1, 5: 1, 6: 2, 7: 3}[distance]
        groups[where].append(distance)

    def send_group(which):
        for distance in groups[which]:
            factor_copy(distance).start()
            word_copy(distance).start()

    sub = lax.broadcasted_iota(jnp.int32, (ROWS, cz), 0)
    lane = lax.broadcasted_iota(jnp.int32, (ROWS, cz), 1)
    first_row, last_row = sub == 0, sub == ROWS - 1
    first_lane, last_lane = lane == 0, lane == cz - 1

    def tile(field, x, t):
        return cur[field, x + 1, pl.ds(t * ROWS, ROWS), :]

    def z_before(value):
        return jnp.where(first_lane, 0.0, pltpu.roll(value, 1, 1))

    def z_after(value):
        return jnp.where(last_lane, 0.0, pltpu.roll(value, cz - 1, 1))

    def y_before(value, field, x, t, slot):
        row = halo_y[slot, pl.ds(x, 1), :] if t == 0 else cur[field, x + 1, pl.ds(t * ROWS - 1, 1), :]
        return jnp.where(first_row, jnp.broadcast_to(row, value.shape), pltpu.roll(value, 1, 0))

    def y_after(value, field, x, t, slot):
        row = halo_y[slot, pl.ds(x, 1), :] if t == tiles - 1 else cur[field, x + 1, pl.ds(t * ROWS + ROWS, 1), :]
        return jnp.where(last_row, jnp.broadcast_to(row, value.shape), pltpu.roll(value, ROWS - 1, 0))

    def velocity(step, x):
        slot = 6 * step
        for t in range(tiles):
            rows = pl.ds(t * ROWS, ROWS)
            scaled = COURANT * coef[0, x, rows, :]
            sxy, sxz, syz = tile(SXY, x, t), tile(SXZ, x, t), tile(SYZ, x, t)
            sxx, syy, szz = tile(SXX, x, t), tile(SYY, x, t), tile(SZZ, x, t)
            moved = (
                tile(VX, x, t) - scaled * (
                    (tile(SXX, x + 1, t) - sxx) + (sxy - y_before(sxy, SXY, x, t, slot + 1)) + (sxz - z_before(sxz))),
                tile(VY, x, t) - scaled * (
                    (sxy - tile(SXY, x - 1, t)) + (y_after(syy, SYY, x, t, slot) - syy) + (syz - z_before(syz))),
                tile(VZ, x, t) - scaled * (
                    (sxz - tile(SXZ, x - 1, t)) + (syz - y_before(syz, SYZ, x, t, slot + 2)) + (z_after(szz) - szz)))
            for field, value in enumerate(moved):
                cur[field, x + 1, rows, :] = value
                if step == STEPS - 1:
                    out[field, x, rows, :] = value

    def stress(step, x):
        slot = 6 * step + 3
        for t in range(tiles):
            rows = pl.ds(t * ROWS, ROWS)
            vx, vy, vz = tile(VX, x, t), tile(VY, x, t), tile(VZ, x, t)
            exx = vx - tile(VX, x - 1, t)
            eyy = vy - y_before(vy, VY, x, t, slot + 2)
            ezz = vz - z_before(vz)
            exy = (y_after(vx, VX, x, t, slot) - vx) + (tile(VY, x + 1, t) - vy)
            exz = (z_after(vx) - vx) + (tile(VZ, x + 1, t) - vz)
            eyz = (z_after(vy) - vy) + (y_after(vz, VZ, x, t, slot + 1) - vz)
            both = (exx, eyy, ezz, exy, exz, eyz)
            for index, value in enumerate(both):
                strain[6 * step + index, x, rows, :] = value
            pull = (COURANT * coef[1, x, rows, :]) * (exx + eyy + ezz)
            mu = COURANT * coef[2, x, rows, :]
            for index, value in enumerate(both):
                change = pull + (2.0 * mu) * value if index < 3 else mu * value
                moved = tile(SXX + index, x, t) - change
                if step == STEPS - 1:
                    out[SXX + index, x, rows, :] = moved
                else:
                    cur[SXX + index, x + 1, rows, :] = moved

    def over(first, last, body):
        def run(x, carry):
            body(x)
            return carry
        lax.fori_loop(first, last, run, 0)

    def ends(body):
        def run(index, carry):
            body(index * (cx - 1))
            return carry
        lax.fori_loop(0, 2, run, 0)

    for step in range(STEPS):
        if step == 0:
            send_x(0, STRESS_X, first_layer)
            for copy in loads:
                copy.wait()
            send_rows(0, STRESS_Y)
            send_group(0)
            def invert(block, carry):
                total = jnp.int32(0)
                for holder in range(n_x):
                    total = jnp.where(perm[0, holder] == block, holder, total)
                inv[block] = total
                return carry
            lax.fori_loop(0, n_x, invert, 0)
        receive(step, STRESS_X, STRESS_Y)
        if step > 0:
            finish_sends(step - 1, SPEED_X, SPEED_Y)
        ends(functools.partial(velocity, step))
        send_x(step, SPEED_X, layer)
        over(1, cx - 1, functools.partial(velocity, step))
        send_rows(step, SPEED_Y)
        send_group(1 + 2 * step)
        receive(step, SPEED_X, SPEED_Y)
        finish_sends(step, STRESS_X, STRESS_Y)
        ends(functools.partial(stress, step))
        if step < STEPS - 1:
            send_x(step + 1, STRESS_X, layer)
        over(1, cx - 1, functools.partial(stress, step))
        if step < STEPS - 1:
            send_rows(step + 1, STRESS_Y)
            send_group(2 + 2 * step)
    finish_sends(STEPS - 1, SPEED_X, SPEED_Y)
    own_words.wait()
    own_factor.wait()
    for distance in range(1, n_x):
        factor_copy(distance).wait()
    to_scalar = pltpu.make_async_copy(factors, factor_s, loc_sem.at[2])
    to_scalar.start()
    for distance in range(1, n_x):
        word_copy(distance).wait()
    to_scalar.wait()

    width = lanes
    per_x = cy * cz // (4 * segw)

    def source(row, chunk):
        offset = row * cz + chunk * width
        within = offset % (4 * segw)
        return offset // (4 * segw), within % segw, within // segw

    sub_w = lax.broadcasted_iota(jnp.int32, (ROWS, width), 0)

    def gradient(x):
        made = {}
        for t in range(tiles):
            for chunk in range(cz // width):
                rows = pl.ds(t * ROWS, ROWS)
                columns = pl.ds(chunk * width, width)
                plan = [source(t * ROWS + r, chunk) for r in range(ROWS)]
                shift = jnp.full((ROWS, width), 8 * plan[0][2], jnp.int32)
                for r in range(1, ROWS):
                    if plan[r][2] != plan[r - 1][2]:
                        shift = jnp.where(sub_w >= r, 8 * plan[r][2], shift)
                key = tuple(p[:2] for p in plan)
                distinct = list(dict.fromkeys(key))
                masks = []
                for item in distinct[1:]:
                    mask = None
                    for r in range(ROWS):
                        if key[r] == item:
                            mask = (sub_w == r) if mask is None else mask | (sub_w == r)
                    masks.append(mask)
                holders = {b: inv[x * per_x + b] for b in dict.fromkeys(k[0] for k in key)}
                blocks = [k[0] for k in key]

                def stored(c):
                    if (key, c) not in made:
                        word = None
                        for position, (block, start) in enumerate(distinct):
                            piece = jnp.broadcast_to(
                                words[holders[block], c, pl.ds(start // lanes, 1), :], (ROWS, width))
                            word = piece if word is None else jnp.where(masks[position - 1], piece, word)
                        made[key, c] = word ^ jnp.int32(-2147483648)
                    byte = (lax.shift_right_logical(made[key, c], shift) & 255) - 128
                    factor = None
                    for r in range(ROWS):
                        if r == 0:
                            factor = factor_s[holders[blocks[0]], 0, c]
                        elif blocks[r] != blocks[r - 1]:
                            factor = jnp.where(sub_w >= r, factor_s[holders[blocks[r]], 0, c], factor)
                    return byte.astype(jnp.float32) * factor

                grad_lambda = jnp.zeros((ROWS, width), jnp.float32)
                grad_mu = jnp.zeros((ROWS, width), jnp.float32)
                for step in range(comp // 6):
                    e = [strain[6 * step + index, x, rows, columns] for index in range(6)]
                    f = [stored(6 * step + index) for index in range(6)]
                    grad_lambda = grad_lambda + (e[0] + e[1] + e[2]) * (f[0] + f[1] + f[2])
                    grad_mu = grad_mu + 2.0 * (e[0] * f[0] + e[1] * f[1] + e[2] * f[2])
                    grad_mu = grad_mu + e[3] * f[3] + e[4] * f[4] + e[5] * f[5]
                grads[0, x, rows, columns] = grad_lambda
                grads[1, x, rows, columns] = grad_mu

    over(0, cx, gradient)


def on_device(n_x, n_y, adjoint, buoyancy, lame_lambda, shear_mu, packed, scales, perm):
    fields, cx, cy, cz = adjoint.shape
    comp, segw = packed.shape[3:]
    lanes = min(128, segw)
    packed = packed.reshape(n_x, comp, segw // lanes, lanes)
    halos = 6 * STEPS
    dma = pltpu.SemaphoreType.DMA
    return pl.pallas_call(
        functools.partial(kernel, n_x, n_y),
        out_shape=(pltpu.VMEM(adjoint.shape, jnp.float32), pltpu.VMEM((2, cx, cy, cz), jnp.float32)),
        in_specs=[pl.BlockSpec(memory_space=pltpu.HBM)] * 6 + [pl.BlockSpec(memory_space=pltpu.SMEM)],
        out_specs=(pl.BlockSpec(memory_space=pltpu.VMEM),) * 2,
        scratch_shapes=[
            pltpu.VMEM((fields, cx + 2, cy, cz), jnp.float32),
            pltpu.VMEM((3, cx, cy, cz), jnp.float32),
            pltpu.VMEM((comp, cx, cy, cz), jnp.float32),
            pltpu.VMEM((halos, cy, cz), jnp.float32),
            pltpu.VMEM((halos, cx, cz), jnp.float32),
            pltpu.VMEM((halos, cx, cz), jnp.float32),
            pltpu.VMEM((n_x, comp, segw // lanes, lanes), jnp.int32),
            pltpu.VMEM((n_x, 1, comp), jnp.float32),
            pltpu.SMEM((n_x, 1, comp), jnp.float32),
            pltpu.SMEM((n_x,), jnp.int32),
            dma((12,)), dma((halos,)), dma((halos,)), dma((halos,)), dma((halos,)),
            dma((n_x,)), dma((n_x,)), dma((n_x,)), dma((n_x,)), dma((3,)),
        ],
        compiler_params=pltpu.CompilerParams(collective_id=0, has_side_effects=True,
                                             vmem_limit_bytes=64000000),
    )(adjoint, buoyancy, lame_lambda, shear_mu, packed, scales, perm)


def solution(mesh):
    return jax.shard_map(
        functools.partial(on_device, mesh.shape["gx"], mesh.shape["gy"]),
        mesh=mesh,
        in_specs=(
            P(None, "gx", "gy", None),
            P("gx", "gy", None),
            P("gx", "gy", None),
            P("gx", "gy", None),
            P("gx", None, "gy", None, None),
            P("gx", None, "gy", None),
            P("gx", None),
        ),
        out_specs=(P(None, "gx", "gy", None), P(None, "gx", "gy", None)),
        check_vma=False,
    )
```

```python
import functools

import jax
import jax.numpy as jnp
from jax import lax
from jax.experimental import pallas as pl
from jax.experimental.pallas import tpu as pltpu
from jax.sharding import PartitionSpec as P

MESH = pl.DeviceIdType.MESH
STEPS = 2
COURANT = 0.15
ROWS = 8
PIECES = 2

VX, VY, VZ, SXX, SYY, SZZ, SXY, SXZ, SYZ = range(9)

STRESS_X = ((0, (SXX,), -1), (1, (SXY, SXZ), 1))
STRESS_Y = ((0, (SYY,), -1), (1, (SXY, SYZ), 1))
SPEED_X = ((3, (VY, VZ), -1), (5, (VX,), 1))
SPEED_Y = ((3, (VX, VZ), -1), (5, (VY,), 1))


def partner(me, distance, count):
    if count & (count - 1):
        return lax.rem(me + distance, count)
    result, bit = me, 1
    while bit < count:
        if distance & bit:
            result = result + bit - 2 * bit * ((me // bit) % 2)
        bit *= 2
    return result


def kernel(n_x, n_y, adj, buoy, lam, shear, packed, scales, perm, out, grads,
           cur, coef, strain, halo_x, halo_y, send_y, factors, factor_s, inv,
           in_sem, xs_sem, xr_sem, ys_sem, yr_sem, ws_sem, wr_sem, fs_sem, fr_sem, loc_sem, *words):
    cx, cy, cz = buoy.shape
    comp = packed.shape[1]
    per_step = comp // STEPS
    lanes = packed.shape[3]
    segw = packed.shape[2] * lanes
    tiles = cy // ROWS
    pieces = xs_sem.shape[1]
    part = cy // pieces
    me_x, me_y = lax.axis_index("gx"), lax.axis_index("gy")

    loads = []
    for index in (SXX, SXY, SXZ, SYY, SYZ, SZZ, VX, VY, VZ):
        loads.append(pltpu.make_async_copy(adj.at[index], cur.at[index, pl.ds(1, cx)], in_sem.at[index]))
    for index, ref in enumerate((buoy, lam, shear)):
        loads.append(pltpu.make_async_copy(ref, coef.at[index], in_sem.at[9 + index]))
    own_words = [pltpu.make_async_copy(packed.at[me_x, pl.ds(step * per_step, per_step)], words[step].at[me_x],
                                       loc_sem.at[2 + step]) for step in range(STEPS)]
    own_factor = pltpu.make_async_copy(scales.at[0, me_x], factors.at[me_x], loc_sem.at[1])
    for copy in loads:
        copy.start()
    for copy in own_words:
        copy.start()
    own_factor.start()

    barrier = pltpu.get_barrier_semaphore()
    for distance in range(1, n_x):
        pl.semaphore_signal(barrier, inc=1, device_id={"gx": partner(me_x, distance, n_x)}, device_id_type=MESH)

    def edge(way, axis):
        me, count = (me_x, n_x) if axis == "gx" else (me_y, n_y)
        return (me > 0) if way < 0 else (me < count - 1)

    for way in (-1, 1):
        @pl.when(edge(way, "gy"))
        def _():
            pl.semaphore_signal(barrier, inc=1, device_id={"gy": me_y + way}, device_id_type=MESH)

    pl.semaphore_wait(barrier, n_x - 1 + jnp.minimum(me_y, 1) + jnp.minimum(n_y - 1 - me_y, 1))

    def copy_x(step, message, source, piece):
        start, fields, way = message
        slot = 6 * step + start
        return pltpu.make_async_remote_copy(
            src_ref=source(fields, way, piece),
            dst_ref=halo_x.at[pl.ds(slot, len(fields)), pl.ds(piece * part, part)],
            send_sem=xs_sem.at[slot, piece], recv_sem=xr_sem.at[slot, piece],
            device_id={"gx": me_x + way}, device_id_type=MESH)

    def copy_y(step, message):
        start, fields, way = message
        slot = 6 * step + start
        return pltpu.make_async_remote_copy(
            src_ref=send_y.at[pl.ds(slot, len(fields))], dst_ref=halo_y.at[pl.ds(slot, len(fields))],
            send_sem=ys_sem.at[slot], recv_sem=yr_sem.at[slot],
            device_id={"gy": me_y + way}, device_id_type=MESH)

    def layer(fields, way, piece):
        return cur.at[pl.ds(fields[0], len(fields)), 1 if way < 0 else cx, pl.ds(piece * part, part)]

    def first_layer(fields, way, piece):
        return adj.at[pl.ds(fields[0], len(fields)), 0 if way < 0 else cx - 1, pl.ds(piece * part, part)]

    def word_copy(distance, step):
        to = partner(me_x, distance, n_x)
        stored = pl.ds(step * per_step, per_step)
        return pltpu.make_async_remote_copy(
            src_ref=packed.at[to, stored], dst_ref=words[step].at[me_x], send_sem=ws_sem.at[distance, step],
            recv_sem=wr_sem.at[distance, step], device_id={"gx": to}, device_id_type=MESH)

    def factor_copy(distance):
        to = partner(me_x, distance, n_x)
        return pltpu.make_async_remote_copy(
            src_ref=scales.at[0, to], dst_ref=factors.at[me_x], send_sem=fs_sem.at[distance],
            recv_sem=fr_sem.at[distance], device_id={"gx": to}, device_id_type=MESH)

    def send_x(step, messages, source, piece):
        for message in messages:
            @pl.when(edge(message[2], "gx"))
            def _():
                copy_x(step, message, source, piece).start()

    def send_rows(step, messages):
        for message in messages:
            start, fields, way = message

            @pl.when(edge(way, "gy"))
            def _():
                row = 0 if way < 0 else cy - 1
                for offset, field in enumerate(fields):
                    for x in range(cx):
                        send_y[6 * step + start + offset, pl.ds(x, 1), :] = cur[field, 1 + x, pl.ds(row, 1), :]
                copy_y(step, message).start()

    def finish_sends(step, messages_x, messages_y):
        for message in messages_x:
            @pl.when(edge(message[2], "gx"))
            def _():
                for piece in range(pieces):
                    copy_x(step, message, layer, piece).wait_send()
        for message in messages_y:
            @pl.when(edge(message[2], "gy"))
            def _():
                copy_y(step, message).wait_send()

    def receive_y(step, messages):
        for message in messages:
            start, fields, way = message

            @pl.when(edge(-way, "gy"))
            def _():
                copy_y(step, message).wait_recv()

            @pl.when(jnp.logical_not(edge(-way, "gy")))
            def _():
                for offset in range(len(fields)):
                    halo_y[6 * step + start + offset] = jnp.zeros((cx, cz), jnp.float32)

    def receive_x(step, messages, piece):
        rows = pl.ds(piece * part, part)
        for message in messages:
            start, fields, way = message
            place = cx + 1 if way < 0 else 0

            @pl.when(edge(-way, "gx"))
            def _():
                copy_x(step, message, layer, piece).wait_recv()
                for offset, field in enumerate(fields):
                    cur[field, place, rows, :] = halo_x[6 * step + start + offset, rows, :]

            @pl.when(jnp.logical_not(edge(-way, "gx")))
            def _():
                for field in fields:
                    cur[field, place, rows, :] = jnp.zeros((part, cz), jnp.float32)

    far = max(3 * n_x // 4, 1)

    def send_group(which):
        step, late = which // 2, which % 2
        for distance in range(2, n_x) if n_x > 2 else ():
            if (distance >= far) == (late == 1):
                word_copy(distance, step).start()
        if late == 1:
            word_copy(1, step).start()
        if which == 0:
            for distance in range(1, n_x):
                factor_copy(distance).start()

    def receive_words(step):
        if step == 0:
            own_factor.wait()
            for distance in range(1, n_x):
                factor_copy(distance).wait()
            to_scalar = pltpu.make_async_copy(factors, factor_s, loc_sem.at[0])
            to_scalar.start()
            to_scalar.wait()
        own_words[step].wait()
        for distance in range(1, n_x):
            word_copy(distance, step).wait()

    sub = lax.broadcasted_iota(jnp.int32, (ROWS, cz), 0)
    lane = lax.broadcasted_iota(jnp.int32, (ROWS, cz), 1)
    first_row, last_row = sub == 0, sub == ROWS - 1
    first_lane, last_lane = lane == 0, lane == cz - 1

    def tile(field, x, t):
        return cur[field, x + 1, pl.ds(t * ROWS, ROWS), :]

    def z_before(value):
        return jnp.where(first_lane, 0.0, pltpu.roll(value, 1, 1))

    def z_after(value):
        return jnp.where(last_lane, 0.0, pltpu.roll(value, cz - 1, 1))

    def y_before(value, field, x, t, slot):
        row = halo_y[slot, pl.ds(x, 1), :] if t == 0 else cur[field, x + 1, pl.ds(t * ROWS - 1, 1), :]
        return jnp.where(first_row, jnp.broadcast_to(row, value.shape), pltpu.roll(value, 1, 0))

    def y_after(value, field, x, t, slot):
        row = halo_y[slot, pl.ds(x, 1), :] if t == tiles - 1 else cur[field, x + 1, pl.ds(t * ROWS + ROWS, 1), :]
        return jnp.where(last_row, jnp.broadcast_to(row, value.shape), pltpu.roll(value, ROWS - 1, 0))

    def velocity(step, which, x):
        slot = 6 * step
        for t in which:
            rows = pl.ds(t * ROWS, ROWS)
            scaled = COURANT * coef[0, x, rows, :]
            sxy, sxz, syz = tile(SXY, x, t), tile(SXZ, x, t), tile(SYZ, x, t)
            sxx, syy, szz = tile(SXX, x, t), tile(SYY, x, t), tile(SZZ, x, t)
            moved = (
                tile(VX, x, t) - scaled * (
                    (tile(SXX, x + 1, t) - sxx) + (sxy - y_before(sxy, SXY, x, t, slot + 1)) + (sxz - z_before(sxz))),
                tile(VY, x, t) - scaled * (
                    (sxy - tile(SXY, x - 1, t)) + (y_after(syy, SYY, x, t, slot) - syy) + (syz - z_before(syz))),
                tile(VZ, x, t) - scaled * (
                    (sxz - tile(SXZ, x - 1, t)) + (syz - y_before(syz, SYZ, x, t, slot + 2)) + (z_after(szz) - szz)))
            for field, value in enumerate(moved):
                cur[field, x + 1, rows, :] = value
                if step == STEPS - 1:
                    out[field, x, rows, :] = value

    def stress(step, which, x):
        slot = 6 * step + 3
        for t in which:
            rows = pl.ds(t * ROWS, ROWS)
            vx, vy, vz = tile(VX, x, t), tile(VY, x, t), tile(VZ, x, t)
            exx = vx - tile(VX, x - 1, t)
            eyy = vy - y_before(vy, VY, x, t, slot + 2)
            ezz = vz - z_before(vz)
            exy = (y_after(vx, VX, x, t, slot) - vx) + (tile(VY, x + 1, t) - vy)
            exz = (z_after(vx) - vx) + (tile(VZ, x + 1, t) - vz)
            eyz = (z_after(vy) - vy) + (y_after(vz, VZ, x, t, slot + 1) - vz)
            both = (exx, eyy, ezz, exy, exz, eyz)
            for index, value in enumerate(both):
                strain[6 * step + index, x, rows, :] = value
            pull = (COURANT * coef[1, x, rows, :]) * (exx + eyy + ezz)
            mu = COURANT * coef[2, x, rows, :]
            for index, value in enumerate(both):
                change = pull + (2.0 * mu) * value if index < 3 else mu * value
                moved = tile(SXX + index, x, t) - change
                if step == STEPS - 1:
                    out[SXX + index, x, rows, :] = moved
                else:
                    cur[SXX + index, x + 1, rows, :] = moved

    def over(first, last, body):
        def run(x, carry):
            body(x)
            return carry
        lax.fori_loop(first, last, run, 0)

    def ends(body):
        def run(index, carry):
            body(index * (cx - 1))
            return carry
        lax.fori_loop(0, 2, run, 0)

    width = lanes
    per_x = cy * cz // (4 * segw)

    def source(row, chunk):
        offset = row * cz + chunk * width
        within = offset % (4 * segw)
        return offset // (4 * segw), within % segw, within // segw

    sub_w = lax.broadcasted_iota(jnp.int32, (ROWS, width), 0)

    def gradient(step, x):
        made = {}
        for t in range(tiles):
            for chunk in range(cz // width):
                rows = pl.ds(t * ROWS, ROWS)
                columns = pl.ds(chunk * width, width)
                plan = [source(t * ROWS + r, chunk) for r in range(ROWS)]
                shift = jnp.full((ROWS, width), 8 * plan[0][2], jnp.int32)
                for r in range(1, ROWS):
                    if plan[r][2] != plan[r - 1][2]:
                        shift = jnp.where(sub_w >= r, 8 * plan[r][2], shift)
                key = tuple(p[:2] for p in plan)
                distinct = list(dict.fromkeys(key))
                masks = []
                for item in distinct[1:]:
                    mask = None
                    for r in range(ROWS):
                        if key[r] == item:
                            mask = (sub_w == r) if mask is None else mask | (sub_w == r)
                    masks.append(mask)
                holders = {b: inv[x * per_x + b] for b in dict.fromkeys(k[0] for k in key)}
                blocks = [k[0] for k in key]

                def stored(c):
                    if (key, c) not in made:
                        word = None
                        for position, (block, start) in enumerate(distinct):
                            piece = jnp.broadcast_to(
                                words[step][holders[block], c - per_step * step, pl.ds(start // lanes, 1), :], (ROWS, width))
                            word = piece if word is None else jnp.where(masks[position - 1], piece, word)
                        made[key, c] = word ^ jnp.int32(-2147483648)
                    byte = (lax.shift_right_logical(made[key, c], shift) & 255) - 128
                    factor = None
                    for r in range(ROWS):
                        if r == 0:
                            factor = factor_s[holders[blocks[0]], 0, c]
                        elif blocks[r] != blocks[r - 1]:
                            factor = jnp.where(sub_w >= r, factor_s[holders[blocks[r]], 0, c], factor)
                    return byte.astype(jnp.float32) * factor

                e = [strain[6 * step + index, x, rows, columns] for index in range(6)]
                f = [stored(6 * step + index) for index in range(6)]
                grad_lambda = (e[0] + e[1] + e[2]) * (f[0] + f[1] + f[2])
                grad_mu = 2.0 * (e[0] * f[0] + e[1] * f[1] + e[2] * f[2])
                grad_mu = grad_mu + e[3] * f[3] + e[4] * f[4] + e[5] * f[5]
                if step > 0:
                    grad_lambda = grads[0, x, rows, columns] + grad_lambda
                    grad_mu = grads[1, x, rows, columns] + grad_mu
                grads[0, x, rows, columns] = grad_lambda
                grads[1, x, rows, columns] = grad_mu

    def inside(piece):
        return range(piece * part // ROWS, (piece + 1) * part // ROWS)

    outer = (0, tiles - 1) if tiles > 1 else (0,)
    inner = range(1, tiles - 1)

    for step in range(STEPS):
        if step == 0:
            for piece in range(pieces):
                send_x(0, STRESS_X, first_layer, piece)
            for copy in loads:
                copy.wait()
            send_rows(0, STRESS_Y)
            send_group(0)
            def invert(block, carry):
                total = jnp.int32(0)
                for holder in range(n_x):
                    total = jnp.where(perm[0, holder] == block, holder, total)
                inv[block] = total
                return carry
            lax.fori_loop(0, n_x, invert, 0)
        if step > 0:
            finish_sends(step - 1, SPEED_X, SPEED_Y)
        receive_y(step, STRESS_Y)
        for piece in range(pieces):
            receive_x(step, STRESS_X, piece)
            ends(functools.partial(velocity, step, inside(piece)))
            send_x(step, SPEED_X, layer, piece)
        over(1, cx - 1, functools.partial(velocity, step, outer))
        send_rows(step, SPEED_Y)
        over(1, cx - 1, functools.partial(velocity, step, inner))
        send_group(1 + 2 * step)
        if step > 0:
            receive_words(step - 1)
            over(0, cx, functools.partial(gradient, step - 1))
        finish_sends(step, STRESS_X, STRESS_Y)
        receive_y(step, SPEED_Y)
        for piece in range(pieces):
            receive_x(step, SPEED_X, piece)
            ends(functools.partial(stress, step, inside(piece)))
            if step < STEPS - 1:
                send_x(step + 1, STRESS_X, layer, piece)
        over(1, cx - 1, functools.partial(stress, step, outer))
        if step < STEPS - 1:
            send_rows(step + 1, STRESS_Y)
        over(1, cx - 1, functools.partial(stress, step, inner))
        if step < STEPS - 1:
            send_group(2 + 2 * step)
    finish_sends(STEPS - 1, SPEED_X, SPEED_Y)
    receive_words(STEPS - 1)
    over(0, cx, functools.partial(gradient, STEPS - 1))


def on_device(n_x, n_y, adjoint, buoyancy, lame_lambda, shear_mu, packed, scales, perm):
    fields, cx, cy, cz = adjoint.shape
    comp, segw = packed.shape[3:]
    lanes = min(128, segw)
    packed = packed.reshape(n_x, comp, segw // lanes, lanes)
    halos = 6 * STEPS
    pieces = PIECES if cy % (PIECES * ROWS) == 0 else 1
    dma = pltpu.SemaphoreType.DMA
    return pl.pallas_call(
        functools.partial(kernel, n_x, n_y),
        out_shape=(pltpu.VMEM(adjoint.shape, jnp.float32), pltpu.VMEM((2, cx, cy, cz), jnp.float32)),
        in_specs=[pl.BlockSpec(memory_space=pltpu.HBM)] * 6 + [pl.BlockSpec(memory_space=pltpu.SMEM)],
        out_specs=(pl.BlockSpec(memory_space=pltpu.VMEM),) * 2,
        scratch_shapes=[
            pltpu.VMEM((fields, cx + 2, cy, cz), jnp.float32),
            pltpu.VMEM((3, cx, cy, cz), jnp.float32),
            pltpu.VMEM((comp, cx, cy, cz), jnp.float32),
            pltpu.VMEM((halos, cy, cz), jnp.float32),
            pltpu.VMEM((halos, cx, cz), jnp.float32),
            pltpu.VMEM((halos, cx, cz), jnp.float32),
            pltpu.VMEM((n_x, 1, comp), jnp.float32),
            pltpu.SMEM((n_x, 1, comp), jnp.float32),
            pltpu.SMEM((n_x,), jnp.int32),
            dma((12,)), dma((halos, pieces)), dma((halos, pieces)), dma((halos,)), dma((halos,)),
            dma((n_x, STEPS)), dma((n_x, STEPS)), dma((n_x,)), dma((n_x,)), dma((2 + STEPS,)),
        ] + [pltpu.VMEM((n_x, comp // STEPS, segw // lanes, lanes), jnp.int32)] * STEPS,
        compiler_params=pltpu.CompilerParams(collective_id=0, has_side_effects=True,
                                             vmem_limit_bytes=64000000),
    )(adjoint, buoyancy, lame_lambda, shear_mu, packed, scales, perm)


def solution(mesh):
    return jax.shard_map(
        functools.partial(on_device, mesh.shape["gx"], mesh.shape["gy"]),
        mesh=mesh,
        in_specs=(
            P(None, "gx", "gy", None),
            P("gx", "gy", None),
            P("gx", "gy", None),
            P("gx", "gy", None),
            P("gx", None, "gy", None, None),
            P("gx", None, "gy", None),
            P("gx", None),
        ),
        out_specs=(P(None, "gx", "gy", None), P(None, "gx", "gy", None)),
        check_vma=False,
    )
```
